8 devices in a mesh: z: 2 (over z, y), y: 2 (over x), x: 2 (over core).
Axes of the slice: x: 2, y: 2, z: 1, core: 2. Of those that a mesh axis runs over, the one named last changes fastest.
Arguments:
- x_in: bfloat16 [32768, 8192], P(('z', 'y', 'x'))
- g_out: bfloat16 [32768, 512], P(('z', 'y', 'x'))
- w_in: bfloat16 [8192, 512], replicated
- w_up1: bfloat16 [512, 2048], replicated
- w_down1: bfloat16 [2048, 512], replicated
- w_up2: bfloat16 [512, 2048], replicated
- w_down2: bfloat16 [2048, 512], replicated
Outputs:
- output 1: bfloat16 [32768, 8192], P(('z', 'y', 'x'))
- output 2: float32 [8192, 512], replicated
- output 3: float32 [512, 2048], replicated
- output 4: float32 [2048, 512], replicated
- output 5: float32 [512, 2048], replicated
- output 6: float32 [2048, 512], replicated
All inputs are finite; a program needn't handle non-finite values.
Results may differ from the reference program's by a relative error of at most 0.0133388.
Values are sent between devices in bfloat16 or wider.
A program may use at most 1 GiB of HBM per device.

```python
import jax
import jax.numpy as jnp
from jax import lax

D_MODEL = 512
D_FF = 2048
D_IN = 8192
TOK_DEV = 4096
N_DEVICES = 8

TOKENS = TOK_DEV * N_DEVICES
SQRT_HALF = 0.7071067811865476
INV_SQRT_TAU = 0.3989422804014327


def gelu_value(pre_act):
    pre_wide = pre_act.astype(jnp.float32)
    return 0.5 * pre_wide * (1.0 + lax.erf(pre_wide * SQRT_HALF))


def gelu_slope(pre_act):
    pre_wide = pre_act.astype(jnp.float32)
    return 0.5 * (1.0 + lax.erf(pre_wide * SQRT_HALF)) + pre_wide * jnp.exp(-0.5 * pre_wide * pre_wide) * INV_SQRT_TAU


def setup_inputs(seed: int = 0) -> dict:
    keys = jax.random.split(jax.random.key(seed), 7)
    x_in = jax.random.normal(keys[0], (TOKENS, D_IN), jnp.float32)
    g_out = jax.random.normal(keys[1], (TOKENS, D_MODEL), jnp.float32)
    w_in = jax.random.normal(keys[2], (D_IN, D_MODEL), jnp.float32) * D_IN ** -0.5
    w_up1 = jax.random.normal(keys[3], (D_MODEL, D_FF), jnp.float32) * D_MODEL ** -0.5
    w_down1 = jax.random.normal(keys[4], (D_FF, D_MODEL), jnp.float32) * D_FF ** -0.5
    w_up2 = jax.random.normal(keys[5], (D_MODEL, D_FF), jnp.float32) * D_MODEL ** -0.5
    w_down2 = jax.random.normal(keys[6], (D_FF, D_MODEL), jnp.float32) * D_FF ** -0.5
    return {
        "x_in": x_in.astype(jnp.bfloat16),
        "g_out": g_out.astype(jnp.bfloat16),
        "w_in": w_in.astype(jnp.bfloat16),
        "w_up1": w_up1.astype(jnp.bfloat16),
        "w_down1": w_down1.astype(jnp.bfloat16),
        "w_up2": w_up2.astype(jnp.bfloat16),
        "w_down2": w_down2.astype(jnp.bfloat16),
    }


def local_backward(x_in, g_out, w_in, w_up1, w_down1, w_up2, w_down2):
    x_mid = jnp.dot(x_in, w_in, preferred_element_type=jnp.float32).astype(jnp.bfloat16)
    pre_one = jnp.dot(x_mid, w_up1, preferred_element_type=jnp.float32).astype(jnp.bfloat16)
    act_one = gelu_value(pre_one).astype(jnp.bfloat16)
    hid_two = (jnp.dot(act_one, w_down1, preferred_element_type=jnp.float32) + x_mid.astype(jnp.float32)).astype(jnp.bfloat16)
    pre_three = jnp.dot(hid_two, w_up2, preferred_element_type=jnp.float32).astype(jnp.bfloat16)
    act_three = gelu_value(pre_three).astype(jnp.bfloat16)
    grad_down2 = jnp.dot(act_three.T, g_out, preferred_element_type=jnp.float32)
    d_act3 = jnp.dot(g_out, w_down2.T, preferred_element_type=jnp.float32).astype(jnp.bfloat16)
    d_pre3 = (d_act3.astype(jnp.float32) * gelu_slope(pre_three)).astype(jnp.bfloat16)
    grad_up2 = jnp.dot(hid_two.T, d_pre3, preferred_element_type=jnp.float32)
    d_hid2 = (jnp.dot(d_pre3, w_up2.T, preferred_element_type=jnp.float32) + g_out.astype(jnp.float32)).astype(jnp.bfloat16)
    grad_down1 = jnp.dot(act_one.T, d_hid2, preferred_element_type=jnp.float32)
    d_act1 = jnp.dot(d_hid2, w_down1.T, preferred_element_type=jnp.float32).astype(jnp.bfloat16)
    d_pre1 = (d_act1.astype(jnp.float32) * gelu_slope(pre_one)).astype(jnp.bfloat16)
    grad_up1 = jnp.dot(x_mid.T, d_pre1, preferred_element_type=jnp.float32)
    d_mid = (jnp.dot(d_pre1, w_up1.T, preferred_element_type=jnp.float32) + d_hid2.astype(jnp.float32)).astype(jnp.bfloat16)
    grad_in = jnp.dot(x_in.T, d_mid, preferred_element_type=jnp.float32)
    dx_rows = jnp.dot(d_mid, w_in.T, preferred_element_type=jnp.float32).astype(jnp.bfloat16)
    return dx_rows, (grad_in, grad_up1, grad_down1, grad_up2, grad_down2)


def reference(x_in, g_out, w_in, w_up1, w_down1, w_up2, w_down2):
    x_shards = x_in.reshape(N_DEVICES, TOK_DEV, D_IN)
    g_shards = g_out.reshape(N_DEVICES, TOK_DEV, D_MODEL)
    zero_sums = (
        jnp.zeros((D_IN, D_MODEL), jnp.float32),
        jnp.zeros((D_MODEL, D_FF), jnp.float32),
        jnp.zeros((D_FF, D_MODEL), jnp.float32),
        jnp.zeros((D_MODEL, D_FF), jnp.float32),
        jnp.zeros((D_FF, D_MODEL), jnp.float32),
    )

    def shard_step(partial_sums, shard):
        dx_rows, grads = local_backward(shard[0], shard[1], w_in, w_up1, w_down1, w_up2, w_down2)
        return tuple(total + piece for total, piece in zip(partial_sums, grads)), dx_rows

    totals, dx_parts = lax.scan(shard_step, zero_sums, (x_shards, g_shards))
    scale = 1.0 / N_DEVICES
    return (dx_parts.reshape(TOKENS, D_IN), totals[0] * scale, totals[1] * scale, totals[2] * scale, totals[3] * scale, totals[4] * scale)
```

```python
import jax
import jax.numpy as jnp
from jax import lax
from jax.sharding import PartitionSpec as P

SQRT_HALF = 0.7071067811865476
INV_SQRT_TAU = 0.3989422804014327
AXES = ("z", "y", "x")
SWAP = [(0, 1), (1, 0)]


def gelu_value(pre_act):
    pre_wide = pre_act.astype(jnp.float32)
    return 0.5 * pre_wide * (1.0 + lax.erf(pre_wide * SQRT_HALF))


def gelu_slope(pre_act):
    pre_wide = pre_act.astype(jnp.float32)
    return 0.5 * (1.0 + lax.erf(pre_wide * SQRT_HALF)) + pre_wide * jnp.exp(-0.5 * pre_wide * pre_wide) * INV_SQRT_TAU


def plain_product(first_op, second_op):
    return lax.dot_general(first_op, second_op, (((1,), (0,)), ((), ())), preferred_element_type=jnp.float32)


def rows_contract(first_op, second_op):
    return lax.dot_general(first_op, second_op, (((0,), (0,)), ((), ())), preferred_element_type=jnp.float32)


def times_transposed(first_op, second_op):
    return lax.dot_general(first_op, second_op, (((1,), (1,)), ((), ())), preferred_element_type=jnp.float32)


def pick(a, i, axis):
    return lax.dynamic_index_in_dim(a, i, axis, keepdims=False)


def mean_over_devices(grad, scale):
    z, y, x = (lax.axis_index(a) for a in AXES)
    rows, cols = grad.shape
    g = grad.reshape(2, 2, 2, 2, rows // 16, cols)
    swap = lambda a, axis: lax.ppermute(a, axis, SWAP)
    s = pick(g, x, 2) + swap(pick(g, 1 - x, 2), "x")
    a, b = s[:, :, 0], s[:, :, 1]
    a = pick(a, y, 1) + swap(pick(a, 1 - y, 1), "y")
    b = pick(b, z, 0) + swap(pick(b, 1 - z, 0), "z")
    a = pick(a, z, 0) + swap(pick(a, 1 - z, 0), "z")
    b = pick(b, y, 0) + swap(pick(b, 1 - y, 0), "y")
    mine = jnp.concatenate([a, b], 0) * scale
    return lax.all_gather(mine, AXES, axis=0, tiled=True)


def solution(mesh):
    scale = 1.0 / mesh.size
    row_spec = P(AXES, None)
    full_spec = P(None, None)

    def device_step(x_in, g_out, w_in, w_up1, w_down1, w_up2, w_down2):
        mean = lambda g: mean_over_devices(g, scale)
        x_mid = plain_product(x_in, w_in).astype(jnp.bfloat16)
        pre_one = plain_product(x_mid, w_up1).astype(jnp.bfloat16)
        act_one = gelu_value(pre_one).astype(jnp.bfloat16)
        hid_two = (plain_product(act_one, w_down1) + x_mid.astype(jnp.float32)).astype(jnp.bfloat16)
        pre_three = plain_product(hid_two, w_up2).astype(jnp.bfloat16)
        act_three = gelu_value(pre_three).astype(jnp.bfloat16)
        dw_down2 = mean(rows_contract(act_three, g_out))
        d_act3 = times_transposed(g_out, w_down2).astype(jnp.bfloat16)
        d_pre3 = (d_act3.astype(jnp.float32) * gelu_slope(pre_three)).astype(jnp.bfloat16)
        dw_up2 = mean(rows_contract(hid_two, d_pre3))
        d_hid2 = (times_transposed(d_pre3, w_up2) + g_out.astype(jnp.float32)).astype(jnp.bfloat16)
        dw_down1 = mean(rows_contract(act_one, d_hid2))
        d_act1 = times_transposed(d_hid2, w_down1).astype(jnp.bfloat16)
        d_pre1 = (d_act1.astype(jnp.float32) * gelu_slope(pre_one)).astype(jnp.bfloat16)
        dw_up1 = mean(rows_contract(x_mid, d_pre1))
        d_mid = (times_transposed(d_pre1, w_up1) + d_hid2.astype(jnp.float32)).astype(jnp.bfloat16)
        quarters = [mean(rows_contract(x_in[:, q * 2048:(q + 1) * 2048], d_mid)) for q in range(4)]
        dw_in = jnp.concatenate(quarters, 0)
        dx_rows = times_transposed(d_mid, w_in).astype(jnp.bfloat16)
        return dx_rows, dw_in, dw_up1, dw_down1, dw_up2, dw_down2

    return jax.shard_map(
        device_step,
        mesh=mesh,
        in_specs=(row_spec, row_spec, full_spec, full_spec, full_spec, full_spec, full_spec),
        out_specs=(row_spec, full_spec, full_spec, full_spec, full_spec, full_spec),
        check_vma=False,
    )
```
